512 devices in a mesh: groups: 2 (over y), gx: 32 (over z), gy: 4 (over x), gz: 2 (over core).
Axes of the slice: x: 4, y: 2, z: 32, core: 2. Of those that a mesh axis runs over, the one named last changes fastest.
The devices are a block of a 4x8x32 slice.
Arguments:
- coords: float32 [64, 16, 16, 3, 128], P(('groups', 'gx'), 'gy', 'gz'), parts along dimension 0, may hold values from 0 to 1.1
- charges: float32 [64, 16, 16, 128], P(('groups', 'gx'), 'gy', 'gz'), parts along dimension 0, may hold values from -2 to 2
- atom_types: int32 [64, 16, 16, 128], P(('groups', 'gx'), 'gy', 'gz'), parts along dimension 0, may hold values from 0 to 63
- counts: int32 [64, 16, 16], P(('groups', 'gx'), 'gy', 'gz'), parts along dimension 0, may hold values from 64 to 128
- c6_table: float32 [64, 64], replicated, may hold values from 0.0001 to 0.001
- c12_table: float32 [64, 64], replicated, may hold values from 1e-08 to 1e-07
Outputs:
- forces: float32 [64, 16, 16, 3, 128], P(('groups', 'gx'), 'gy', 'gz'), parts along dimension 0
- energy: float32 [2], P('groups'), parts along dimension 0
The draws below stay inside these ranges and needn't reach their ends.
There are 2 independent parts, one for each index of `groups`. The reference program is written for one: setup_inputs(seed, part) draws one part's arguments, and reference() takes and returns one part's arrays. A program takes and returns all parts, laid end to end along the dimension named above; an argument that names none is the same for every part. Nothing has to cross between parts.
All inputs are finite; a program needn't handle non-finite values.
Results may differ from the reference program's by a relative error of at most 0.0003.
Values sent between devices are 32-bit elements; how exact they have to be, the bound alone decides.
A program may use at most 64 MiB of HBM per device.

```python
import math
import jax
import jax.numpy as jnp
from jax import lax

SLOTS = 128
TYPES = 64
NX = 32
NY = 16
NZ = 16


def set_ends(result, stream_key, low, top_value):
    index_at = [jax.random.randint(jax.random.fold_in(stream_key, axis), (), 0, length) for axis, length in enumerate(result.shape)]
    widest = result.shape.index(max(result.shape))
    beside = index_at[:widest] + [(index_at[widest] + 1) % result.shape[widest]] + index_at[widest + 1:]
    return result.at[tuple(index_at)].set(low).at[tuple(beside)].set(top_value)


def steps_of(key, extent, cuts, least, top_value):
    factor_of = 1.0
    for position, blocks in cuts:
        draws = jax.random.uniform(jax.random.fold_in(jax.random.fold_in(key, 6), position), (blocks,), jnp.float32, least / len(cuts), top_value / len(cuts))
        factor_of = factor_of * jnp.repeat(jnp.exp(draws), extent[position] // blocks).reshape((-1,) + (1,) * (len(extent) - 1 - position))
    return factor_of


def bell_draw(own_key, dims, scale, reach, split=(), kind=jnp.bfloat16):
    level = steps_of(own_key, dims, split, -0.22, 0.18) if split else 1.0
    result = jax.random.normal(own_key, dims, jnp.float32) * scale * level
    return jnp.minimum(jnp.maximum(result, -reach), reach).astype(kind)


def setup_inputs(seed: int = 0, part: int = 0) -> dict:
    streams_of = jax.random.split(jax.random.key(seed), 7)
    own_keys = jax.random.split(jax.random.fold_in(streams_of[6], part), 7)
    return {
        "coords": jnp.clip(1.1 * jax.random.uniform(own_keys[0], (NX, NY, NZ, 3, SLOTS), jnp.float32) ** steps_of(own_keys[0], (NX, NY, NZ, 3, SLOTS), ((0, 32), (1, 4), (2, 2)), -0.2, 0.2), 0.0, 1.1),
        "charges": bell_draw(own_keys[1], (NX, NY, NZ, SLOTS), 0.4, 2.0, ((0, 32), (1, 4), (2, 2)), jnp.float32),
        "atom_types": set_ends(jax.random.randint(own_keys[2], (NX, NY, NZ, SLOTS), 0, TYPES), jax.random.fold_in(own_keys[2], 1), 0, TYPES - 1).astype(jnp.int32),
        "counts": set_ends(jax.random.randint(own_keys[3], (NX, NY, NZ), SLOTS // 2, SLOTS + 1), jax.random.fold_in(own_keys[3], 1), SLOTS // 2, SLOTS).astype(jnp.int32),
        "c6_table": jnp.clip(jnp.exp(jax.random.uniform(streams_of[4], (TYPES, TYPES), jnp.float32, math.log(0.0001), math.log(0.001))), 0.0001, 0.001),
        "c12_table": jnp.clip(jnp.exp(jax.random.uniform(streams_of[5], (TYPES, TYPES), jnp.float32, math.log(9.99999993922529e-09), math.log(1.0000000116860974e-07))), 9.99999993922529e-09, 1.0000000116860974e-07),
    }


CELL_EDGE = 1.1
CUT_SQUARE = 1.0
SOFTEN = 0.09
ENERGY_UNIT = 0.1
CELL_PAIRS = ((0, 1), (0, 2), (0, 3), (0, 4), (0, 5), (0, 6), (0, 7), (1, 2), (1, 4), (2, 4), (1, 6), (2, 5), (4, 3))

def corner_bits(corner_index):
    return (corner_index >> 2 & 1, corner_index >> 1 & 1, corner_index & 1)

def pack_cells(coords, charges, atom_types, counts):
    slot_count = coords.shape[-1]
    occupied = (jnp.arange(slot_count, dtype=jnp.int32) < counts[..., None]).astype(jnp.float32)
    return jnp.concatenate([coords, charges[..., None, :], atom_types.astype(jnp.float32)[..., None, :], occupied[..., None, :]], axis=3)

def tile_terms(pack_a, pack_b, c6_sym, c12_sym, offset, pair_mask):
    type_ids = jnp.arange(c6_sym.shape[0]).astype(jnp.float32)
    type_hot_a = (pack_a[4][:, None] == type_ids[None, :]).astype(jnp.float32)
    type_hot_b = (pack_b[4][:, None] == type_ids[None, :]).astype(jnp.float32)
    c6_pair = jnp.dot(jnp.dot(type_hot_a, c6_sym, precision=lax.Precision.HIGHEST), type_hot_b.T, precision=lax.Precision.HIGHEST)
    c12_pair = jnp.dot(jnp.dot(type_hot_a, c12_sym, precision=lax.Precision.HIGHEST), type_hot_b.T, precision=lax.Precision.HIGHEST)
    charge_pair = pack_a[3][:, None] * pack_b[3][None, :]
    occupied_pair = pack_a[5][:, None] * pack_b[5][None, :] * pair_mask
    edge_inverse = 1.0 / (CUT_SQUARE + SOFTEN)
    edge_cube = edge_inverse ** 3

    def pair_energy(position_a, position_b):
        separation = position_b[:, None, :] - position_a[:, :, None] + offset[:, None, None]
        dist_square = lax.optimization_barrier(jnp.sum(separation * separation, axis=0))
        inverse = 1.0 / (dist_square + SOFTEN)
        inverse_cube = inverse * inverse * inverse
        coulomb = charge_pair * (jnp.sqrt(inverse) - edge_inverse ** 0.5)
        dispersion = c12_pair * (inverse_cube * inverse_cube - edge_cube * edge_cube) - c6_pair * (inverse_cube - edge_cube)
        cutoff_taper = jnp.maximum(1.0 - dist_square / CUT_SQUARE, 0.0)
        return ENERGY_UNIT * jnp.sum((coulomb + dispersion) * cutoff_taper * cutoff_taper * occupied_pair)
    energy, (grad_a, grad_b) = jax.value_and_grad(pair_energy, argnums=(0, 1))(pack_a[:3], pack_b[:3])
    return (energy, -grad_a, -grad_b)

def cell_batch(packs_a, packs_b, c6_sym, c12_sym, offset, pair_mask):

    def single(tiles):
        return tile_terms(tiles[0], tiles[1], c6_sym, c12_sym, offset, pair_mask)
    return lax.map(single, (packs_a, packs_b), batch_size=8)

def reference(coords, charges, atom_types, counts, c6_table, c12_table):
    c6_sym = 0.5 * (c6_table + c6_table.T)
    c12_sym = 0.5 * (c12_table + c12_table.T)
    packed = pack_cells(coords, charges, atom_types, counts)
    grid_shape = packed.shape[:3]
    slot_count = packed.shape[-1]
    upper_pairs = jnp.triu(jnp.ones((slot_count, slot_count), jnp.float32), 1)
    all_pairs = jnp.ones((slot_count, slot_count), jnp.float32)
    forces = jnp.zeros(grid_shape + (3, slot_count), jnp.float32)
    energy_sum = jnp.zeros((), jnp.float32)
    for source, target in ((0, 0),) + CELL_PAIRS:
        corner_a = corner_bits(source)
        corner_b = corner_bits(target)
        cells_a = jnp.roll(packed, (-corner_a[0], -corner_a[1], -corner_a[2]), axis=(0, 1, 2))
        cells_b = jnp.roll(packed, (-corner_b[0], -corner_b[1], -corner_b[2]), axis=(0, 1, 2))
        offset = jnp.array([(corner_b[k] - corner_a[k]) * CELL_EDGE for k in range(3)], jnp.float32)
        pair_mask = upper_pairs if source == target else all_pairs
        energies, force_a, force_b = cell_batch(cells_a.reshape((-1, 6, slot_count)), cells_b.reshape((-1, 6, slot_count)), c6_sym, c12_sym, offset, pair_mask)
        force_a = jnp.roll(force_a.reshape(grid_shape + (3, slot_count)), corner_a, axis=(0, 1, 2))
        force_b = jnp.roll(force_b.reshape(grid_shape + (3, slot_count)), corner_b, axis=(0, 1, 2))
        forces = forces + force_a + force_b
        energy_sum = energy_sum + jnp.sum(energies)
    return (forces, energy_sum.reshape(1))
```

```python
import functools

import jax
import jax.numpy as jnp
import numpy as np
from jax import lax
from jax.experimental import pallas as pl
from jax.experimental.pallas import tpu as pltpu
from jax.sharding import PartitionSpec as P

CELL_EDGE = 1.1
SOFTEN = 0.09
ENERGY_UNIT = 0.1
EDGE_INVERSE = 1.0 / (1.0 + SOFTEN)
EDGE_ROOT = EDGE_INVERSE**0.5
EDGE_CUBE = EDGE_INVERSE**3
NEIGHBOURS = (
    (0, 0, 1),
    (0, 1, 0),
    (0, 1, 1),
    (1, 0, 0),
    (1, 0, 1),
    (1, 1, 0),
    (1, 1, 1),
    (0, 1, -1),
    (1, 0, -1),
    (1, 1, -1),
    (1, -1, 0),
    (1, -1, 1),
    (1, -1, -1),
)


def neighbour_lists(ny, nz):
    tiles, ranges = [], []
    empty = 2 * (ny + 1) * (nz + 1)
    for y in range(ny + 1):
        for z in range(nz + 1):
            p = y * (nz + 1) + z
            partners = [(p, 0)] if y < ny and z < nz else []
            for ox, oy, oz in NEIGHBOURS:
                low_y, low_z = y + min(oy, 0), z + min(oz, 0)
                if 0 <= low_y < ny and 0 <= low_z < nz:
                    partners.append(((ox * (ny + 1) + y + oy) * (nz + 1) + z + oz, -1024))
            if len(partners) % 2:
                partners.append((empty, -1024))
            ranges.append((len(tiles) // 2, len(partners) // 2))
            tiles += [(p, b, below) for b, below in partners]
    tiles.append((0, empty, 0))
    return np.array(tiles, np.int32).reshape(-1), np.array(ranges, np.int32).reshape(-1)


def split(value):
    high = value.astype(jnp.bfloat16)
    return high, (value - high.astype(jnp.float32)).astype(jnp.bfloat16)


def pair_kernel(
    shape, tile_ref, range_ref, raw_ref, table_ref, force_ref, energy_ref,
    pack_ref, col_ref, left_ref, right_ref, acc_a, acc_b, even_ref, odd_ref,
):
    iota = functools.partial(lax.broadcasted_iota, jnp.int32, (128, 128))
    row = lax.broadcasted_iota(jnp.int32, (8, 128), 0)
    cells_a, cells = shape[1] * shape[2], shape[0] * shape[1] * shape[2]

    for x in range(shape[0]):
        for y in range(shape[1]):
            for z in range(shape[2]):
                place = jnp.where(row == 0, x, jnp.where(row == 1, y, jnp.where(row == 2, z, 0)))
                pack_ref[(x * shape[1] + y) * shape[2] + z] = raw_ref[x, y, z] + CELL_EDGE * place
    pack_ref[cells] = jnp.where(row == 4, 64.0, 0.0)

    def prepare_a(p):
        turned = jnp.transpose(pack_ref[p])
        for f in range(3):
            col_ref[p, f] = jnp.broadcast_to(turned[:, f : f + 1], (128, 128))
        qa = jnp.broadcast_to(turned[:, 3:4], (128, 128))
        col_ref[p, 3] = qa * (1.0 / 6.0)
        kinds = jnp.broadcast_to(turned[:, 4:5], (128, 128))
        hot = jnp.where(kinds == iota(1).astype(jnp.float32), 1.0, 0.0).astype(jnp.bfloat16)
        rows = jnp.dot(
            jnp.concatenate([hot, hot], axis=1), table_ref[...], preferred_element_type=jnp.float32
        )
        r6, r12 = rows[:, :128], rows[:, 128:]
        low_half = iota(1) < 64
        empty = jnp.zeros((128, 128), jnp.bfloat16)

        def halves(value):
            high = value.astype(jnp.bfloat16).astype(jnp.float32)
            return jnp.where(low_half, high, value - high).astype(jnp.bfloat16)

        left_ref[p, :128, :128] = halves(r6)
        left_ref[p, :128, 128:] = empty
        left_ref[p, 128:256, :128] = halves(r12)
        left_ref[p, 128:256, 128:] = empty
        left_ref[p, 256:, :128] = halves(EDGE_CUBE * EDGE_CUBE * r12 - EDGE_CUBE * r6)
        qs = qa * EDGE_ROOT
        high = qs.astype(jnp.bfloat16).astype(jnp.float32)
        lane = iota(1)
        left_ref[p, 256:, 128:] = jnp.where(
            lane < 4, jnp.where((lane & 1) == 0, high, qs - high), 0.0
        ).astype(jnp.bfloat16)
        acc_a[p] = jnp.zeros((3, 128, 128), jnp.float32)

    def prepare_b(b):
        kinds = jnp.broadcast_to(pack_ref[b, pl.ds(4, 1), :].astype(jnp.int32), (128, 128))
        hot = jnp.where((iota(0) & 63) == kinds, 1.0, 0.0)
        right_ref[b, :128] = hot.astype(jnp.bfloat16)
        q = jnp.broadcast_to(pack_ref[b, pl.ds(3, 1), :], (16, 128))
        high = q.astype(jnp.bfloat16).astype(jnp.float32)
        row = lax.broadcasted_iota(jnp.int32, (16, 128), 0)
        q = jnp.where(row < 2, high, jnp.where(row < 4, q - high, 0.0))
        right_ref[b, 128:144] = q.astype(jnp.bfloat16)
        right_ref[b, 144:] = jnp.zeros((112, 128), jnp.bfloat16)
        acc_b[b] = jnp.zeros((3, 8, 128), jnp.float32)

    step = 3

    @pl.loop(0, cells_a // step)
    def _(i):
        for j in range(step):
            prepare_a(i * step + j)

    @pl.loop(0, cells // 5)
    def _(i):
        for j in range(5):
            prepare_b(i * 5 + j)

    prepare_b(cells)
    energy_ref[...] = jnp.zeros((8, 128), jnp.float32)

    def look_up(t, out_ref):
        p, b = tile_ref[3 * t], tile_ref[3 * t + 1]
        out_ref[...] = jnp.dot(left_ref[p], right_ref[b], preferred_element_type=jnp.float32)

    def tile(p, t, rows, in_ref, masked):
        b = tile_ref[3 * t + 1]
        xb, yb, zb, qb = (pack_ref[b, pl.ds(f, 1), :] for f in range(4))
        energy = jnp.zeros((8, 128), jnp.float32)
        other = [jnp.zeros((8, 128), jnp.float32)] * 3
        for first in range(0, rows, 8):
            at = slice(first, first + 8)
            xa, ya, za, qa = (col_ref[p, f, at, :] for f in range(4))
            c6 = in_ref[first : first + 8, :]
            c12 = in_ref[128 + first : 136 + first, :]
            edge = in_ref[256 + first : 264 + first, :]
            dx, dy, dz = xb - xa, yb - ya, zb - za
            r2 = dx * dx + dy * dy + dz * dz
            w = jnp.maximum(1.0 - r2, 0.0)
            if masked:
                least = tile_ref[3 * t + 2] + first
                apart = lax.broadcasted_iota(jnp.int32, (8, 128), 1) - lax.broadcasted_iota(
                    jnp.int32, (8, 128), 0
                )
                w = jnp.where(apart > least, w, 0.0)
            s = lax.rsqrt(r2 + SOFTEN)
            v = s * s
            v3 = v * v * v
            m = c12 * v3
            lj = (m - c6) * v3
            coulomb6 = (qa * qb) * s
            u = 6.0 * coulomb6 + (lj - edge)
            slope = coulomb6 + (lj + m * v3)
            uw = u * w
            energy = energy + uw * w
            g = w * ((1.5 * (w * v)) * slope + u)
            for c, d in enumerate((dx, dy, dz)):
                f = g * d
                other[c] = other[c] + f
                acc_a[p, c, at, :] += f
        for c in range(3):
            acc_b[b, c] += other[c]
        energy_ref[...] += energy

    look_up(0, even_ref)

    @pl.loop(0, cells_a)
    def _(p):
        filled = pack_ref[p, pl.ds(5, 1), pl.ds(0, 1)][0, 0].astype(jnp.int32)
        first, pairs = range_ref[2 * p], range_ref[2 * p + 1]

        def two(i, rows, masked):
            t = 2 * i
            look_up(t + 1, odd_ref)
            tile(p, t, rows, even_ref, masked)
            look_up(t + 2, even_ref)
            tile(p, t + 1, rows, odd_ref, False)

        for rows in range(64, 129, 16):
            fits = filled <= rows
            if rows > 64:
                fits = fits & (filled > rows - 16)

            @pl.when(fits)
            def _(rows=rows):
                two(first, rows, True)

                @pl.loop(1, pairs)
                def _(i):
                    two(first + i, rows, False)

    def sublane_sums(block):
        return jnp.concatenate(
            [jnp.sum(block[c], axis=0, keepdims=True) for c in range(3)]
            + [jnp.zeros((5, 128), jnp.float32)],
            axis=0,
        )

    scale = 4.0 * ENERGY_UNIT

    def finish_a(p):
        turned = [jnp.transpose(acc_a[p, c]) for c in range(3)]
        return (sublane_sums(acc_b[p]) - sublane_sums(turned)) * scale

    @pl.loop(0, shape[1])
    def _(i):
        for j in range(shape[2]):
            force_ref[0, i, j] = finish_a(i * shape[2] + j)

    @pl.loop(0, shape[1])
    def _(i):
        for j in range(shape[2]):
            force_ref[1, i, j] = sublane_sums(acc_b[cells_a + i * shape[2] + j]) * scale


def pair_forces(lists, raw, table):
    tiles, ranges = lists
    shape = raw.shape[:3]
    cells_a = shape[1] * shape[2]
    cells = cells_a * shape[0]
    vmem = pl.BlockSpec(memory_space=pltpu.VMEM)
    smem = pl.BlockSpec(memory_space=pltpu.SMEM)
    return pl.pallas_call(
        functools.partial(pair_kernel, shape),
        out_shape=(
            jax.ShapeDtypeStruct(raw.shape, jnp.float32),
            jax.ShapeDtypeStruct((8, 128), jnp.float32),
        ),
        in_specs=[smem, smem, vmem, vmem],
        out_specs=(vmem, vmem),
        scratch_shapes=[
            pltpu.VMEM((cells + 1, 8, 128), jnp.float32),
            pltpu.VMEM((cells_a, 4, 128, 128), jnp.float32),
            pltpu.VMEM((cells_a, 384, 256), jnp.bfloat16),
            pltpu.VMEM((cells + 1, 256, 128), jnp.bfloat16),
            pltpu.VMEM((cells_a, 3, 128, 128), jnp.float32),
            pltpu.VMEM((cells + 1, 3, 8, 128), jnp.float32),
            pltpu.VMEM((384, 128), jnp.float32),
            pltpu.VMEM((384, 128), jnp.float32),
        ],
        compiler_params=pltpu.CompilerParams(vmem_limit_bytes=56 * 1024 * 1024),
    )(tiles, ranges, raw, table)


AXES = ("gx", "gy", "gz")
CORNERS = ((1, 0, 0), (0, 1, 0), (0, 0, 1), (1, 1, 0), (1, 0, 1), (0, 1, 1), (1, 1, 1))
REACH = 4


def device_at(sizes, offset):
    return {
        axis: lax.rem(lax.axis_index(axis) + offset[k] % sizes[k], sizes[k])
        for k, axis in enumerate(AXES)
        if offset[k] % sizes[k]
    }


def greet(sizes, offsets):
    both = {tuple(o % n for o, n in zip(f, sizes)) for f in offsets}
    both |= {tuple(-o % n for o, n in zip(f, sizes)) for f in offsets}
    both = sorted(both)
    barrier = pltpu.get_barrier_semaphore()
    for offset in both:
        pl.semaphore_signal(
            barrier, inc=1, device_id=device_at(sizes, offset), device_id_type=pl.DeviceIdType.MESH
        )
    pl.semaphore_wait(barrier, len(both))


def send(source, target, send_sem, receive_sem, device):
    copy = pltpu.make_async_remote_copy(
        src_ref=source,
        dst_ref=target,
        send_sem=send_sem,
        recv_sem=receive_sem,
        device_id=device,
        device_id_type=pl.DeviceIdType.MESH,
    )
    copy.start()
    return copy


def import_kernel(sizes, own_ref, whole_ref, local_sem, send_sem, receive_sem):
    ny, nz = own_ref.shape[:2]
    local = pltpu.make_async_copy(own_ref, whole_ref.at[0, pl.ds(0, ny), pl.ds(0, nz)], local_sem)
    local.start()
    greet(sizes, CORNERS)
    copies = []
    for k, (x, y, z) in enumerate(CORNERS):
        ty, tz = (1 if y else ny), (1 if z else nz)
        copies.append(
            send(
                own_ref.at[pl.ds(0, ty), pl.ds(0, tz)],
                whole_ref.at[x, pl.ds(ny if y else 0, ty), pl.ds(nz if z else 0, tz)],
                send_sem.at[k],
                receive_sem.at[k],
                device_at(sizes, (-x, -y, -z)),
            )
        )
    local.wait()
    for copy in copies:
        copy.wait()


def import_cells(own):
    ny, nz = own.shape[:2]
    sizes = tuple(lax.axis_size(a) for a in AXES)
    vmem = pl.BlockSpec(memory_space=pltpu.VMEM)
    return pl.pallas_call(
        functools.partial(import_kernel, sizes),
        out_shape=jax.ShapeDtypeStruct((2, ny + 1, nz + 1) + own.shape[2:], jnp.float32),
        in_specs=[vmem],
        out_specs=vmem,
        scratch_shapes=[
            pltpu.SemaphoreType.DMA,
            pltpu.SemaphoreType.DMA((len(CORNERS),)),
            pltpu.SemaphoreType.DMA((len(CORNERS),)),
        ],
        compiler_params=pltpu.CompilerParams(collective_id=0, has_side_effects=True),
    )(own)


def export_kernel(
    sizes, force_ref, energy_ref, total_ref, sum_ref,
    r0, r1, r2, r3, r4, r5, r6, line_ref, column_ref, plane_ref,
    send_sem, receive_sem, line_send, line_receive, plane_send, plane_receive,
):
    nx, gy, gz = sizes
    ny, nz = total_ref.shape[:2]
    arrivals = (r0, r1, r2, r3, r4, r5, r6)
    plane = [(0, y, z) for y in range(gy) for z in range(gz) if (y, z) != (0, 0)]
    centre = nx // 2 - 1
    greet(sizes, list(CORNERS) + [(d, 0, 0) for d in range(1, REACH + 1)] + plane)
    lines = []

    def line(source, target, offset):
        k = len(lines)
        lines.append(
            send(source, target, line_send.at[k], line_receive.at[k], device_at(sizes, (offset, 0, 0)))
        )

    for d in range(1, REACH + 1):
        line(energy_ref, line_ref.at[centre + d], -d)
        line(energy_ref, line_ref.at[centre - d], d)
    copies = []
    for k, (x, y, z) in enumerate(CORNERS):
        copies.append(
            send(
                force_ref.at[
                    x, pl.ds(ny if y else 0, 1 if y else ny), pl.ds(nz if z else 0, 1 if z else nz)
                ],
                arrivals[k],
                send_sem.at[k],
                receive_sem.at[k],
                device_at(sizes, (x, y, z)),
            )
        )
    line_ref[centre] = energy_ref[...]
    begun = 0
    for stage in range(1, nx // 2 // REACH):
        waited = len(lines)
        for copy in lines[begun:waited]:
            copy.wait()
        begun = waited
        first = REACH * (stage - 1)
        line(
            line_ref.at[pl.ds(centre + first + 1, REACH)],
            line_ref.at[pl.ds(centre + first + 1 + REACH, REACH)],
            -REACH,
        )
        count = REACH - (1 if stage == nx // 2 // REACH - 1 else 0)
        line(
            line_ref.at[pl.ds(centre - first - count, count)],
            line_ref.at[pl.ds(centre - first - count - REACH, count)],
            REACH,
        )
        if stage == 1:
            for copy in copies:
                copy.wait()
            for y in range(ny):
                for z in range(nz):
                    total = force_ref[0, y, z]
                    for k, (_, cy, cz) in enumerate(CORNERS):
                        if (y == 0 or not cy) and (z == 0 or not cz):
                            total = total + arrivals[k][y, z]
                    total_ref[y, z] = total[:3]
    for copy in lines[begun:]:
        copy.wait()
    me = lax.axis_index("gx")
    column = jnp.zeros((8, 128), jnp.float32)
    for i in range(nx):
        column = column + line_ref[lax.rem(centre + i + nx - me, nx)]
    column_ref[...] = column
    mine = lax.axis_index("gy") * gz + lax.axis_index("gz")
    planes = [
        send(column_ref, plane_ref.at[mine], plane_send.at[k], plane_receive.at[k], device_at(sizes, o))
        for k, o in enumerate(plane)
    ]
    plane_ref[mine] = column
    for copy in planes:
        copy.wait()
    total = plane_ref[0]
    for k in range(1, gy * gz):
        total = total + plane_ref[k]
    sum_ref[...] = jnp.broadcast_to(ENERGY_UNIT * jnp.sum(total, keepdims=True), (8, 128))


def export(forces, energy, slots):
    ny, nz = forces.shape[1] - 1, forces.shape[2] - 1
    sizes = tuple(lax.axis_size(a) for a in AXES)
    vmem = pl.BlockSpec(memory_space=pltpu.VMEM)
    lines = 2 * REACH + 2 * (sizes[0] // 2 // REACH - 1)
    dma = pltpu.SemaphoreType.DMA
    return pl.pallas_call(
        functools.partial(export_kernel, sizes),
        out_shape=(
            jax.ShapeDtypeStruct((ny, nz, 3, slots), jnp.float32),
            jax.ShapeDtypeStruct((8, 128), jnp.float32),
        ),
        in_specs=[vmem, vmem],
        out_specs=(vmem, vmem),
        scratch_shapes=[
            pltpu.VMEM((1 if y else ny, 1 if z else nz, 8, slots), jnp.float32) for _, y, z in CORNERS
        ]
        + [
            pltpu.VMEM((sizes[0], 8, 128), jnp.float32),
            pltpu.VMEM((8, 128), jnp.float32),
            pltpu.VMEM((sizes[1] * sizes[2], 8, 128), jnp.float32),
            dma((len(CORNERS),)),
            dma((len(CORNERS),)),
            dma((lines,)),
            dma((lines,)),
            dma((sizes[1] * sizes[2],)),
            dma((sizes[1] * sizes[2],)),
        ],
        compiler_params=pltpu.CompilerParams(collective_id=1, has_side_effects=True),
    )(forces, energy)


def on_device(coords, charges, atom_types, counts, c6_table, c12_table):
    ny, nz, slots = coords.shape[1], coords.shape[2], coords.shape[4]
    filled = jnp.arange(slots, dtype=jnp.int32) < counts[..., None]
    own = jnp.concatenate(
        [
            coords,
            jnp.where(filled, charges, 0.0)[..., None, :],
            jnp.where(filled, atom_types, 64).astype(jnp.float32)[..., None, :],
            jnp.broadcast_to(counts.astype(jnp.float32)[..., None, None], counts.shape + (1, slots)),
            jnp.zeros(counts.shape + (2, slots), jnp.float32),
        ],
        axis=3,
    )[0]
    raw = import_cells(own)
    types = c6_table.shape[0]
    both = jnp.stack([0.5 * (c6_table + c6_table.T), 0.5 * (c12_table + c12_table.T)], axis=1)
    both = jnp.concatenate([both, both], axis=2)
    both = jnp.pad(both, ((0, 128 - types), (0, 0), (0, 0))).reshape(128, 256)
    high = lax.reduce_precision(both, 8, 7)
    table = jnp.concatenate([high, both - high]).astype(jnp.bfloat16)
    lists = tuple(jnp.asarray(k) for k in neighbour_lists(ny, nz))
    forces, energy = pair_forces(lists, raw, table)
    total, energy_sum = export(forces, energy, slots)
    return (total[None], energy_sum[0, :1])


def solution(mesh):
    return jax.shard_map(
        on_device,
        mesh=mesh,
        in_specs=(
            P(("groups", "gx"), "gy", "gz", None, None),
            P(("groups", "gx"), "gy", "gz", None),
            P(("groups", "gx"), "gy", "gz", None),
            P(("groups", "gx"), "gy", "gz"),
            P(),
            P(),
        ),
        out_specs=(P(("groups", "gx"), "gy", "gz", None, None), P("groups")),
        check_vma=False,
    )
```

```python
import functools

import jax
import jax.numpy as jnp
import numpy as np
from jax import lax
from jax.experimental import pallas as pl
from jax.experimental.pallas import tpu as pltpu
from jax.sharding import PartitionSpec as P

CELL_EDGE = 1.1
SOFTEN = 0.09
ENERGY_UNIT = 0.1
EDGE_INVERSE = 1.0 / (1.0 + SOFTEN)
EDGE_ROOT = EDGE_INVERSE**0.5
EDGE_CUBE = EDGE_INVERSE**3
NEIGHBOURS = (
    (0, 0, 1),
    (0, 1, 0),
    (0, 1, 1),
    (1, 0, 0),
    (1, 0, 1),
    (1, 1, 0),
    (1, 1, 1),
    (0, 1, -1),
    (1, 0, -1),
    (1, 1, -1),
    (1, -1, 0),
    (1, -1, 1),
    (1, -1, -1),
)


def neighbour_lists(ny, nz):
    tiles, ranges = [], []
    empty = 2 * (ny + 1) * (nz + 1)
    for y in range(ny + 1):
        for z in range(nz + 1):
            p = y * (nz + 1) + z
            partners = [(p, 0)] if y < ny and z < nz else []
            for ox, oy, oz in NEIGHBOURS:
                low_y, low_z = y + min(oy, 0), z + min(oz, 0)
                if 0 <= low_y < ny and 0 <= low_z < nz:
                    partners.append(((ox * (ny + 1) + y + oy) * (nz + 1) + z + oz, -1024))
            if len(partners) % 2:
                partners.append((empty, -1024))
            ranges.append((len(tiles) // 2, len(partners) // 2))
            tiles += [(p, b, below) for b, below in partners]
    tiles += [(0, empty, 0)] * 2
    return np.array(tiles, np.int32).reshape(-1), np.array(ranges, np.int32).reshape(-1)


def split(value):
    high = value.astype(jnp.bfloat16)
    return high, (value - high.astype(jnp.float32)).astype(jnp.bfloat16)


def pair_kernel(
    shape, tile_ref, range_ref, raw_ref, table_ref, force_ref, energy_ref,
    pack_ref, col_ref, left_ref, right_ref, acc_a, acc_b, *found,
):
    iota = functools.partial(lax.broadcasted_iota, jnp.int32, (128, 128))
    row = lax.broadcasted_iota(jnp.int32, (8, 128), 0)
    cells_a, cells = shape[1] * shape[2], shape[0] * shape[1] * shape[2]

    for x in range(shape[0]):
        for y in range(shape[1]):
            for z in range(shape[2]):
                place = jnp.where(row == 0, x, jnp.where(row == 1, y, jnp.where(row == 2, z, 0)))
                pack_ref[(x * shape[1] + y) * shape[2] + z] = raw_ref[x, y, z] + CELL_EDGE * place
    pack_ref[cells] = jnp.where(row == 4, 64.0, 0.0)

    def column(p, f):
        return jnp.transpose(jnp.broadcast_to(pack_ref[p, pl.ds(f, 1), :], (128, 128)))

    def prepare_a(p):
        for f in range(4):
            col_ref[p, f] = column(p, f)
        hot = jnp.where(column(p, 4) == iota(1).astype(jnp.float32), 1.0, 0.0).astype(jnp.bfloat16)
        rows = jnp.dot(
            jnp.concatenate([hot, hot], axis=1), table_ref[...], preferred_element_type=jnp.float32
        )
        r6, r12 = rows[:, :128], rows[:, 128:]
        low_half = iota(1) < 64

        def halves(value):
            high = value.astype(jnp.bfloat16).astype(jnp.float32)
            return jnp.where(low_half, high, value - high).astype(jnp.bfloat16)

        for k, value in enumerate((r6, r12, EDGE_CUBE * EDGE_CUBE * r12 - EDGE_CUBE * r6)):
            both = halves(value)
            for first in range(0, 128, 16):
                at = 3 * first + 16 * k
                left_ref[p, at : at + 16] = both[first : first + 16]
        acc_a[p] = jnp.zeros((3, 128, 128), jnp.float32)

    def prepare_b(b):
        kinds = jnp.broadcast_to(pack_ref[b, pl.ds(4, 1), :].astype(jnp.int32), (128, 128))
        right_ref[b] = jnp.where((iota(0) & 63) == kinds, 1.0, 0.0).astype(jnp.bfloat16)
        acc_b[b] = jnp.zeros((3, 8, 128), jnp.float32)

    step = 3

    @pl.loop(0, cells_a // step)
    def _(i):
        for j in range(step):
            prepare_a(i * step + j)

    @pl.loop(0, cells // 5)
    def _(i):
        for j in range(5):
            prepare_b(i * 5 + j)

    prepare_b(cells)
    energy_ref[...] = jnp.zeros((8, 128), jnp.float32)

    def look_up(t, out_ref, rows):
        p, b = tile_ref[3 * t], tile_ref[3 * t + 1]
        out_ref[: 3 * rows] = jnp.dot(
            left_ref[p, : 3 * rows], right_ref[b], preferred_element_type=jnp.float32
        )

    def tile(p, t, rows, in_ref, masked):
        b = tile_ref[3 * t + 1]
        xb, yb, zb, qb = (pack_ref[b, pl.ds(f, 1), :] for f in range(4))
        energy = jnp.zeros((8, 128), jnp.float32)
        other = [jnp.zeros((8, 128), jnp.float32)] * 3
        for first in range(0, rows, 8):
            at = slice(first, first + 8)
            xa, ya, za, qa = (col_ref[p, f, at, :] for f in range(4))
            found_at = 3 * (first - first % 16) + first % 16
            c6, c12, edge = (in_ref[found_at + 16 * k : found_at + 16 * k + 8, :] for k in range(3))
            dx, dy, dz = xb - xa, yb - ya, zb - za
            r2 = dx * dx + dy * dy + dz * dz
            w = jnp.maximum(1.0 - r2, 0.0)
            if masked:
                least = tile_ref[3 * t + 2] + first
                apart = lax.broadcasted_iota(jnp.int32, (8, 128), 1) - lax.broadcasted_iota(
                    jnp.int32, (8, 128), 0
                )
                w = jnp.where(apart > least, w, 0.0)
            s = lax.rsqrt(r2 + SOFTEN)
            v = s * s
            v3 = v * v * v
            m = c12 * v3
            lj = (m - c6) * v3
            charge = qa * qb
            coulomb = charge * s
            u = (coulomb - charge * EDGE_ROOT) + (lj - edge)
            slope = coulomb * (1.0 / 6.0) + (lj + m * v3)
            uw = u * w
            energy = energy + uw * w
            g = w * ((1.5 * (w * v)) * slope + u)
            for c, d in enumerate((dx, dy, dz)):
                f = g * d
                other[c] = other[c] + f
                acc_a[p, c, at, :] += f
        for c in range(3):
            acc_b[b, c] += other[c]
        energy_ref[...] += energy

    for k in range(2):
        look_up(k, found[k], 128)

    @pl.loop(0, cells_a)
    def _(p):
        filled = pack_ref[p, pl.ds(5, 1), pl.ds(0, 1)][0, 0].astype(jnp.int32)
        first, pairs = range_ref[2 * p], range_ref[2 * p + 1]

        def two(i, rows, next_rows):
            for turn in range(2):

                @pl.when((i & 1) == turn)
                def _(turn=turn):
                    for k in range(2):
                        look_up(2 * i + 2 + k, found[2 - 2 * turn + k], next_rows)
                    for k in range(2):
                        tile(p, 2 * i + k, rows, found[2 * turn + k], k == 0)

        steps = (96, 128)
        for least, rows in zip((0,) + steps, steps):
            fits = (filled <= rows) & (filled > least)

            @pl.when(fits)
            def _(rows=rows):
                @pl.loop(0, pairs - 1)
                def _(i):
                    two(first + i, rows, rows)

                two(first + pairs - 1, rows, 128)

    def sublane_sums(block):
        return jnp.concatenate(
            [jnp.sum(block[c], axis=0, keepdims=True) for c in range(3)]
            + [jnp.zeros((5, 128), jnp.float32)],
            axis=0,
        )

    scale = 4.0 * ENERGY_UNIT

    def finish_a(p):
        turned = [jnp.transpose(acc_a[p, c]) for c in range(3)]
        return (sublane_sums(acc_b[p]) - sublane_sums(turned)) * scale

    @pl.loop(0, shape[1])
    def _(i):
        for j in range(shape[2]):
            force_ref[0, i, j] = finish_a(i * shape[2] + j)

    @pl.loop(0, shape[1])
    def _(i):
        for j in range(shape[2]):
            force_ref[1, i, j] = sublane_sums(acc_b[cells_a + i * shape[2] + j]) * scale


def pair_forces(lists, raw, table):
    tiles, ranges = lists
    shape = raw.shape[:3]
    cells_a = shape[1] * shape[2]
    cells = cells_a * shape[0]
    vmem = pl.BlockSpec(memory_space=pltpu.VMEM)
    smem = pl.BlockSpec(memory_space=pltpu.SMEM)
    return pl.pallas_call(
        functools.partial(pair_kernel, shape),
        out_shape=(
            jax.ShapeDtypeStruct(raw.shape, jnp.float32),
            jax.ShapeDtypeStruct((8, 128), jnp.float32),
        ),
        in_specs=[smem, smem, vmem, vmem],
        out_specs=(vmem, vmem),
        scratch_shapes=[
            pltpu.VMEM((cells + 1, 8, 128), jnp.float32),
            pltpu.VMEM((cells_a, 4, 128, 128), jnp.float32),
            pltpu.VMEM((cells_a, 384, 128), jnp.bfloat16),
            pltpu.VMEM((cells + 1, 128, 128), jnp.bfloat16),
            pltpu.VMEM((cells_a, 3, 128, 128), jnp.float32),
            pltpu.VMEM((cells + 1, 3, 8, 128), jnp.float32),
        ]
        + [pltpu.VMEM((384, 128), jnp.float32)] * 4,
        compiler_params=pltpu.CompilerParams(vmem_limit_bytes=56 * 1024 * 1024),
    )(tiles, ranges, raw, table)


AXES = ("gx", "gy", "gz")
CORNERS = ((1, 0, 0), (0, 1, 0), (0, 0, 1), (1, 1, 0), (1, 0, 1), (0, 1, 1), (1, 1, 1))
REACH = 4


def device_at(sizes, offset):
    return {
        axis: lax.rem(lax.axis_index(axis) + offset[k] % sizes[k], sizes[k])
        for k, axis in enumerate(AXES)
        if offset[k] % sizes[k]
    }


def greet(sizes, offsets):
    both = {tuple(o % n for o, n in zip(f, sizes)) for f in offsets}
    both |= {tuple(-o % n for o, n in zip(f, sizes)) for f in offsets}
    both = sorted(both)
    barrier = pltpu.get_barrier_semaphore()
    for offset in both:
        pl.semaphore_signal(
            barrier, inc=1, device_id=device_at(sizes, offset), device_id_type=pl.DeviceIdType.MESH
        )
    pl.semaphore_wait(barrier, len(both))


def send(source, target, send_sem, receive_sem, device):
    copy = pltpu.make_async_remote_copy(
        src_ref=source,
        dst_ref=target,
        send_sem=send_sem,
        recv_sem=receive_sem,
        device_id=device,
        device_id_type=pl.DeviceIdType.MESH,
    )
    copy.start()
    return copy


def import_kernel(sizes, own_ref, whole_ref, send_sem, receive_sem):
    ny, nz = own_ref.shape[:2]
    greet(sizes, CORNERS)
    copies = []
    for k, (x, y, z) in enumerate(CORNERS):
        ty, tz = (1 if y else ny), (1 if z else nz)
        copies.append(
            send(
                own_ref.at[pl.ds(0, ty), pl.ds(0, tz)],
                whole_ref.at[x, pl.ds(ny if y else 0, ty), pl.ds(nz if z else 0, tz)],
                send_sem.at[k],
                receive_sem.at[k],
                device_at(sizes, (-x, -y, -z)),
            )
        )
    whole_ref[0, :ny, :nz] = own_ref[...]
    for copy in copies:
        copy.wait()


def import_cells(own):
    ny, nz = own.shape[:2]
    sizes = tuple(lax.axis_size(a) for a in AXES)
    vmem = pl.BlockSpec(memory_space=pltpu.VMEM)
    return pl.pallas_call(
        functools.partial(import_kernel, sizes),
        out_shape=jax.ShapeDtypeStruct((2, ny + 1, nz + 1) + own.shape[2:], jnp.float32),
        in_specs=[vmem],
        out_specs=vmem,
        scratch_shapes=[
            pltpu.SemaphoreType.DMA((len(CORNERS),)),
            pltpu.SemaphoreType.DMA((len(CORNERS),)),
        ],
        compiler_params=pltpu.CompilerParams(collective_id=0, has_side_effects=True),
    )(own)


def export_kernel(
    sizes, force_ref, energy_ref, total_ref, sum_ref,
    r0, r1, r2, r3, r4, r5, r6, line_ref, column_ref, plane_ref,
    send_sem, receive_sem, line_send, line_receive, plane_send, plane_receive,
):
    nx, gy, gz = sizes
    ny, nz = total_ref.shape[:2]
    arrivals = (r0, r1, r2, r3, r4, r5, r6)
    plane = [(0, y, z) for y in range(gy) for z in range(gz) if (y, z) != (0, 0)]
    centre = nx // 2 - 1
    greet(sizes, list(CORNERS) + [(d, 0, 0) for d in range(1, REACH + 1)] + plane)
    lines = []

    def line(source, target, offset):
        k = len(lines)
        lines.append(
            send(source, target, line_send.at[k], line_receive.at[k], device_at(sizes, (offset, 0, 0)))
        )

    for d in range(1, REACH + 1):
        line(energy_ref, line_ref.at[centre + d], -d)
        line(energy_ref, line_ref.at[centre - d], d)
    copies = []
    for k, (x, y, z) in enumerate(CORNERS):
        copies.append(
            send(
                force_ref.at[
                    x, pl.ds(ny if y else 0, 1 if y else ny), pl.ds(nz if z else 0, 1 if z else nz)
                ],
                arrivals[k],
                send_sem.at[k],
                receive_sem.at[k],
                device_at(sizes, (x, y, z)),
            )
        )
    line_ref[centre] = energy_ref[...]
    begun = 0
    for stage in range(1, nx // 2 // REACH):
        waited = len(lines)
        for copy in lines[begun:waited]:
            copy.wait()
        begun = waited
        first = REACH * (stage - 1)
        line(
            line_ref.at[pl.ds(centre + first + 1, REACH)],
            line_ref.at[pl.ds(centre + first + 1 + REACH, REACH)],
            -REACH,
        )
        count = REACH - (1 if stage == nx // 2 // REACH - 1 else 0)
        line(
            line_ref.at[pl.ds(centre - first - count, count)],
            line_ref.at[pl.ds(centre - first - count - REACH, count)],
            REACH,
        )
        if stage == 1:
            for copy in copies:
                copy.wait()
            for y in range(ny):
                for z in range(nz):
                    total = force_ref[0, y, z]
                    for k, (_, cy, cz) in enumerate(CORNERS):
                        if (y == 0 or not cy) and (z == 0 or not cz):
                            total = total + arrivals[k][y, z]
                    total_ref[y, z] = total[:3]
    for copy in lines[begun:]:
        copy.wait()
    me = lax.axis_index("gx")
    column = jnp.zeros((8, 128), jnp.float32)
    for i in range(nx):
        column = column + line_ref[lax.rem(centre + i + nx - me, nx)]
    column_ref[...] = column
    mine = lax.axis_index("gy") * gz + lax.axis_index("gz")
    planes = [
        send(column_ref, plane_ref.at[mine], plane_send.at[k], plane_receive.at[k], device_at(sizes, o))
        for k, o in enumerate(plane)
    ]
    plane_ref[mine] = column
    for copy in planes:
        copy.wait()
    total = plane_ref[0]
    for k in range(1, gy * gz):
        total = total + plane_ref[k]
    sum_ref[...] = jnp.broadcast_to(ENERGY_UNIT * jnp.sum(total, keepdims=True), (8, 128))


def export(forces, energy, slots):
    ny, nz = forces.shape[1] - 1, forces.shape[2] - 1
    sizes = tuple(lax.axis_size(a) for a in AXES)
    vmem = pl.BlockSpec(memory_space=pltpu.VMEM)
    lines = 2 * REACH + 2 * (sizes[0] // 2 // REACH - 1)
    dma = pltpu.SemaphoreType.DMA
    return pl.pallas_call(
        functools.partial(export_kernel, sizes),
        out_shape=(
            jax.ShapeDtypeStruct((ny, nz, 3, slots), jnp.float32),
            jax.ShapeDtypeStruct((8, 128), jnp.float32),
        ),
        in_specs=[vmem, vmem],
        out_specs=(vmem, vmem),
        scratch_shapes=[
            pltpu.VMEM((1 if y else ny, 1 if z else nz, 8, slots), jnp.float32) for _, y, z in CORNERS
        ]
        + [
            pltpu.VMEM((sizes[0], 8, 128), jnp.float32),
            pltpu.VMEM((8, 128), jnp.float32),
            pltpu.VMEM((sizes[1] * sizes[2], 8, 128), jnp.float32),
            dma((len(CORNERS),)),
            dma((len(CORNERS),)),
            dma((lines,)),
            dma((lines,)),
            dma((sizes[1] * sizes[2],)),
            dma((sizes[1] * sizes[2],)),
        ],
        compiler_params=pltpu.CompilerParams(collective_id=1, has_side_effects=True),
    )(forces, energy)


def on_device(coords, charges, atom_types, counts, c6_table, c12_table):
    ny, nz, slots = coords.shape[1], coords.shape[2], coords.shape[4]
    filled = jnp.arange(slots, dtype=jnp.int32) < counts[..., None]
    own = jnp.concatenate(
        [
            coords,
            jnp.where(filled, charges, 0.0)[..., None, :],
            jnp.where(filled, atom_types, 64).astype(jnp.float32)[..., None, :],
            jnp.broadcast_to(counts.astype(jnp.float32)[..., None, None], counts.shape + (1, slots)),
            jnp.zeros(counts.shape + (2, slots), jnp.float32),
        ],
        axis=3,
    )[0]
    raw = import_cells(own)
    types = c6_table.shape[0]
    both = jnp.stack([0.5 * (c6_table + c6_table.T), 0.5 * (c12_table + c12_table.T)], axis=1)
    both = jnp.concatenate([both, both], axis=2)
    both = jnp.pad(both, ((0, 128 - types), (0, 0), (0, 0))).reshape(128, 256)
    high = lax.reduce_precision(both, 8, 7)
    table = jnp.concatenate([high, both - high]).astype(jnp.bfloat16)
    lists = tuple(jnp.asarray(k) for k in neighbour_lists(ny, nz))
    forces, energy = pair_forces(lists, raw, table)
    total, energy_sum = export(forces, energy, slots)
    return (total[None], energy_sum[0, :1])


def solution(mesh):
    return jax.shard_map(
        on_device,
        mesh=mesh,
        in_specs=(
            P(("groups", "gx"), "gy", "gz", None, None),
            P(("groups", "gx"), "gy", "gz", None),
            P(("groups", "gx"), "gy", "gz", None),
            P(("groups", "gx"), "gy", "gz"),
            P(),
            P(),
        ),
        out_specs=(P(("groups", "gx"), "gy", "gz", None, None), P("groups")),
        check_vma=False,
    )
```

```python
import functools

import jax
import jax.numpy as jnp
import numpy as np
from jax import lax
from jax.experimental import pallas as pl
from jax.experimental.pallas import tpu as pltpu
from jax.sharding import PartitionSpec as P

CELL_EDGE = 1.1
SOFTEN = 0.09
ENERGY_UNIT = 0.1
EDGE_INVERSE = 1.0 / (1.0 + SOFTEN)
EDGE_ROOT = EDGE_INVERSE**0.5
EDGE_CUBE = EDGE_INVERSE**3
NEIGHBOURS = (
    (0, 0, 1),
    (0, 1, 0),
    (0, 1, 1),
    (1, 0, 0),
    (1, 0, 1),
    (1, 1, 0),
    (1, 1, 1),
    (0, 1, -1),
    (1, 0, -1),
    (1, 1, -1),
    (1, -1, 0),
    (1, -1, 1),
    (1, -1, -1),
)


def neighbour_lists(ny, nz):
    tiles, ranges = [], []
    empty = 2 * (ny + 1) * (nz + 1)
    for y in range(ny + 1):
        for z in range(nz + 1):
            p = y * (nz + 1) + z
            partners = [(p, 0)] if y < ny and z < nz else []
            for ox, oy, oz in NEIGHBOURS:
                low_y, low_z = y + min(oy, 0), z + min(oz, 0)
                if 0 <= low_y < ny and 0 <= low_z < nz:
                    partners.append(((ox * (ny + 1) + y + oy) * (nz + 1) + z + oz, -1024))
            if len(partners) % 2:
                partners.append((empty, -1024))
            ranges.append((len(tiles) // 2, len(partners) // 2))
            tiles += [(p, b, below) for b, below in partners]
    tiles += [(0, empty, 0)] * 2
    return np.array(tiles, np.int32).reshape(-1), np.array(ranges, np.int32).reshape(-1)


def split(value):
    high = value.astype(jnp.bfloat16)
    return high, (value - high.astype(jnp.float32)).astype(jnp.bfloat16)


def pair_kernel(
    shape, tile_ref, range_ref, raw_ref, table_ref, force_ref, energy_ref,
    pack_ref, col_ref, left_ref, right_ref, acc_a, acc_b, *found,
):
    iota = functools.partial(lax.broadcasted_iota, jnp.int32, (128, 128))
    row = lax.broadcasted_iota(jnp.int32, (8, 128), 0)
    cells_a, cells = shape[1] * shape[2], shape[0] * shape[1] * shape[2]

    for x in range(shape[0]):
        for y in range(shape[1]):
            for z in range(shape[2]):
                place = jnp.where(row == 0, x, jnp.where(row == 1, y, jnp.where(row == 2, z, 0)))
                pack_ref[(x * shape[1] + y) * shape[2] + z] = raw_ref[x, y, z] + CELL_EDGE * place
    pack_ref[cells] = jnp.where(row == 4, 64.0, 0.0)

    def column(p, f):
        return jnp.transpose(jnp.broadcast_to(pack_ref[p, pl.ds(f, 1), :], (128, 128)))

    def prepare_a(p):
        for f in range(4):
            col_ref[p, f] = column(p, f)
        hot = jnp.where(column(p, 4) == iota(1).astype(jnp.float32), 1.0, 0.0).astype(jnp.bfloat16)
        rows = jnp.dot(
            jnp.concatenate([hot, hot], axis=1), table_ref[...], preferred_element_type=jnp.float32
        )
        r6, r12 = rows[:, :128], rows[:, 128:]
        low_half = iota(1) < 64

        def halves(value):
            high = value.astype(jnp.bfloat16).astype(jnp.float32)
            return jnp.where(low_half, high, value - high).astype(jnp.bfloat16)

        for k, value in enumerate((r6, r12, EDGE_CUBE * EDGE_CUBE * r12 - EDGE_CUBE * r6)):
            both = halves(value)
            for first in range(0, 128, 16):
                at = 3 * first + 16 * k
                left_ref[p, at : at + 16] = both[first : first + 16]
        acc_a[p] = jnp.zeros((3, 128, 128), jnp.float32)

    def prepare_b(b):
        kinds = jnp.broadcast_to(pack_ref[b, pl.ds(4, 1), :].astype(jnp.int32), (128, 128))
        right_ref[b] = jnp.where((iota(0) & 63) == kinds, 1.0, 0.0).astype(jnp.bfloat16)
        acc_b[b] = jnp.zeros((3, 8, 128), jnp.float32)

    step = 3

    @pl.loop(0, cells_a // step)
    def _(i):
        for j in range(step):
            prepare_a(i * step + j)

    @pl.loop(0, cells // 5)
    def _(i):
        for j in range(5):
            prepare_b(i * 5 + j)

    prepare_b(cells)
    energy_ref[...] = jnp.zeros((8, 128), jnp.float32)

    def look_up(t, out_ref, rows):
        p, b = tile_ref[3 * t], tile_ref[3 * t + 1]
        out_ref[: 3 * rows] = jnp.dot(
            left_ref[p, : 3 * rows], right_ref[b], preferred_element_type=jnp.float32
        )

    def tile(p, t, rows, in_ref, masked):
        b = tile_ref[3 * t + 1]
        xb, yb, zb, qb = (pack_ref[b, pl.ds(f, 1), :] for f in range(4))
        energy = jnp.zeros((8, 128), jnp.float32)
        other = [jnp.zeros((8, 128), jnp.float32)] * 3
        for first in range(0, rows, 8):
            at = slice(first, first + 8)
            xa, ya, za, qa = (col_ref[p, f, at, :] for f in range(4))
            found_at = 3 * (first - first % 16) + first % 16
            c6, c12, edge = (in_ref[found_at + 16 * k : found_at + 16 * k + 8, :] for k in range(3))
            dx, dy, dz = xb - xa, yb - ya, zb - za
            r2 = dx * dx + dy * dy + dz * dz
            w = jnp.maximum(1.0 - r2, 0.0)
            if masked:
                least = tile_ref[3 * t + 2] + first
                apart = lax.broadcasted_iota(jnp.int32, (8, 128), 1) - lax.broadcasted_iota(
                    jnp.int32, (8, 128), 0
                )
                w = jnp.where(apart > least, w, 0.0)
            s = lax.rsqrt(r2 + SOFTEN)
            v = s * s
            v3 = v * v * v
            m = c12 * v3
            lj = (m - c6) * v3
            charge = qa * qb
            coulomb = charge * s
            u = (coulomb - charge * EDGE_ROOT) + (lj - edge)
            slope = coulomb * (1.0 / 6.0) + (lj + m * v3)
            uw = u * w
            energy = energy + uw * w
            g = w * ((1.5 * (w * v)) * slope + u)
            for c, d in enumerate((dx, dy, dz)):
                f = g * d
                other[c] = other[c] + f
                acc_a[p, c, at, :] += f
        for c in range(3):
            acc_b[b, c] += other[c]
        energy_ref[...] += energy

    for k in range(2):
        look_up(k, found[k], 128)

    @pl.loop(0, cells_a)
    def _(p):
        filled = pack_ref[p, pl.ds(5, 1), pl.ds(0, 1)][0, 0].astype(jnp.int32)
        first, pairs = range_ref[2 * p], range_ref[2 * p + 1]

        def two(i, rows, next_rows):
            for turn in range(2):

                @pl.when((i & 1) == turn)
                def _(turn=turn):
                    for k in range(2):
                        look_up(2 * i + 2 + k, found[2 - 2 * turn + k], next_rows)
                    for k in range(2):
                        tile(p, 2 * i + k, rows, found[2 * turn + k], k == 0)

        steps = (96, 128)
        for least, rows in zip((0,) + steps, steps):
            fits = (filled <= rows) & (filled > least)

            @pl.when(fits)
            def _(rows=rows):
                @pl.loop(0, pairs - 1)
                def _(i):
                    two(first + i, rows, rows)

                two(first + pairs - 1, rows, 128)

    def sublane_sums(block):
        return jnp.concatenate(
            [jnp.sum(block[c], axis=0, keepdims=True) for c in range(3)]
            + [jnp.zeros((5, 128), jnp.float32)],
            axis=0,
        )

    scale = 4.0 * ENERGY_UNIT

    def finish_a(p):
        turned = [jnp.transpose(acc_a[p, c]) for c in range(3)]
        return (sublane_sums(acc_b[p]) - sublane_sums(turned)) * scale

    @pl.loop(0, shape[1])
    def _(i):
        for j in range(shape[2]):
            force_ref[0, i, j] = finish_a(i * shape[2] + j)

    @pl.loop(0, shape[1])
    def _(i):
        for j in range(shape[2]):
            force_ref[1, i, j] = sublane_sums(acc_b[cells_a + i * shape[2] + j]) * scale


def pair_forces(lists, raw, table):
    tiles, ranges = lists
    shape = raw.shape[:3]
    cells_a = shape[1] * shape[2]
    cells = cells_a * shape[0]
    vmem = pl.BlockSpec(memory_space=pltpu.VMEM)
    smem = pl.BlockSpec(memory_space=pltpu.SMEM)
    return pl.pallas_call(
        functools.partial(pair_kernel, shape),
        out_shape=(
            jax.ShapeDtypeStruct(raw.shape, jnp.float32),
            jax.ShapeDtypeStruct((8, 128), jnp.float32),
        ),
        in_specs=[smem, smem, vmem, vmem],
        out_specs=(vmem, vmem),
        scratch_shapes=[
            pltpu.VMEM((cells + 1, 8, 128), jnp.float32),
            pltpu.VMEM((cells_a, 4, 128, 128), jnp.float32),
            pltpu.VMEM((cells_a, 384, 128), jnp.bfloat16),
            pltpu.VMEM((cells + 1, 128, 128), jnp.bfloat16),
            pltpu.VMEM((cells_a, 3, 128, 128), jnp.float32),
            pltpu.VMEM((cells + 1, 3, 8, 128), jnp.float32),
        ]
        + [pltpu.VMEM((384, 128), jnp.float32)] * 4,
        compiler_params=pltpu.CompilerParams(vmem_limit_bytes=56 * 1024 * 1024),
    )(tiles, ranges, raw, table)


AXES = ("gx", "gy", "gz")
CORNERS = ((1, 0, 0), (0, 1, 0), (0, 0, 1), (1, 1, 0), (1, 0, 1), (0, 1, 1), (1, 1, 1))
REACH = 8


def device_at(sizes, offset):
    return {
        axis: lax.rem(lax.axis_index(axis) + offset[k] % sizes[k], sizes[k])
        for k, axis in enumerate(AXES)
        if offset[k] % sizes[k]
    }


def greet(sizes, offsets):
    both = {tuple(o % n for o, n in zip(f, sizes)) for f in offsets}
    both |= {tuple(-o % n for o, n in zip(f, sizes)) for f in offsets}
    both = sorted(both)
    barrier = pltpu.get_barrier_semaphore()
    for offset in both:
        pl.semaphore_signal(
            barrier, inc=1, device_id=device_at(sizes, offset), device_id_type=pl.DeviceIdType.MESH
        )
    pl.semaphore_wait(barrier, len(both))


def send(source, target, send_sem, receive_sem, device):
    copy = pltpu.make_async_remote_copy(
        src_ref=source,
        dst_ref=target,
        send_sem=send_sem,
        recv_sem=receive_sem,
        device_id=device,
        device_id_type=pl.DeviceIdType.MESH,
    )
    copy.start()
    return copy


def import_kernel(sizes, own_ref, whole_ref, send_sem, receive_sem):
    ny, nz = own_ref.shape[:2]
    greet(sizes, CORNERS)
    copies = []
    for k, (x, y, z) in enumerate(CORNERS):
        ty, tz = (1 if y else ny), (1 if z else nz)
        copies.append(
            send(
                own_ref.at[pl.ds(0, ty), pl.ds(0, tz)],
                whole_ref.at[x, pl.ds(ny if y else 0, ty), pl.ds(nz if z else 0, tz)],
                send_sem.at[k],
                receive_sem.at[k],
                device_at(sizes, (-x, -y, -z)),
            )
        )
    whole_ref[0, :ny, :nz] = own_ref[...]
    for copy in copies:
        copy.wait()


def import_cells(own):
    ny, nz = own.shape[:2]
    sizes = tuple(lax.axis_size(a) for a in AXES)
    vmem = pl.BlockSpec(memory_space=pltpu.VMEM)
    return pl.pallas_call(
        functools.partial(import_kernel, sizes),
        out_shape=jax.ShapeDtypeStruct((2, ny + 1, nz + 1) + own.shape[2:], jnp.float32),
        in_specs=[vmem],
        out_specs=vmem,
        scratch_shapes=[
            pltpu.SemaphoreType.DMA((len(CORNERS),)),
            pltpu.SemaphoreType.DMA((len(CORNERS),)),
        ],
        compiler_params=pltpu.CompilerParams(collective_id=0, has_side_effects=True),
    )(own)


def export_kernel(
    sizes, force_ref, energy_ref, total_ref, sum_ref,
    r0, r1, r2, r3, r4, r5, r6, line_ref, column_ref, plane_ref,
    send_sem, receive_sem, line_send, line_receive, plane_send, plane_receive,
):
    nx, gy, gz = sizes
    ny, nz = total_ref.shape[:2]
    arrivals = (r0, r1, r2, r3, r4, r5, r6)
    plane = [(0, y, z) for y in range(gy) for z in range(gz) if (y, z) != (0, 0)]
    centre = nx // 2 - 1
    greet(sizes, list(CORNERS) + [(d, 0, 0) for d in range(1, REACH + 1)] + plane)
    lines = []

    def line(source, target, offset):
        k = len(lines)
        lines.append(
            send(source, target, line_send.at[k], line_receive.at[k], device_at(sizes, (offset, 0, 0)))
        )

    for d in range(1, REACH + 1):
        line(energy_ref, line_ref.at[centre + d], -d)
        line(energy_ref, line_ref.at[centre - d], d)
    copies = []
    for k, (x, y, z) in enumerate(CORNERS):
        copies.append(
            send(
                force_ref.at[
                    x, pl.ds(ny if y else 0, 1 if y else ny), pl.ds(nz if z else 0, 1 if z else nz)
                ],
                arrivals[k],
                send_sem.at[k],
                receive_sem.at[k],
                device_at(sizes, (x, y, z)),
            )
        )
    line_ref[centre] = energy_ref[...]
    begun = 0
    for stage in range(1, nx // 2 // REACH):
        waited = len(lines)
        for copy in lines[begun:waited]:
            copy.wait()
        begun = waited
        first = REACH * (stage - 1)
        line(
            line_ref.at[pl.ds(centre + first + 1, REACH)],
            line_ref.at[pl.ds(centre + first + 1 + REACH, REACH)],
            -REACH,
        )
        count = REACH - (1 if stage == nx // 2 // REACH - 1 else 0)
        line(
            line_ref.at[pl.ds(centre - first - count, count)],
            line_ref.at[pl.ds(centre - first - count - REACH, count)],
            REACH,
        )
        if stage == 1:
            for copy in copies:
                copy.wait()
            for y in range(ny):
                for z in range(nz):
                    total = force_ref[0, y, z]
                    for k, (_, cy, cz) in enumerate(CORNERS):
                        if (y == 0 or not cy) and (z == 0 or not cz):
                            total = total + arrivals[k][y, z]
                    total_ref[y, z] = total[:3]
    for copy in lines[begun:]:
        copy.wait()
    me = lax.axis_index("gx")
    column = jnp.zeros((8, 128), jnp.float32)
    for i in range(nx):
        column = column + line_ref[lax.rem(centre + i + nx - me, nx)]
    column_ref[...] = column
    mine = lax.axis_index("gy") * gz + lax.axis_index("gz")
    planes = [
        send(column_ref, plane_ref.at[mine], plane_send.at[k], plane_receive.at[k], device_at(sizes, o))
        for k, o in enumerate(plane)
    ]
    plane_ref[mine] = column
    for copy in planes:
        copy.wait()
    total = plane_ref[0]
    for k in range(1, gy * gz):
        total = total + plane_ref[k]
    sum_ref[...] = jnp.broadcast_to(ENERGY_UNIT * jnp.sum(total, keepdims=True), (8, 128))


def export(forces, energy, slots):
    ny, nz = forces.shape[1] - 1, forces.shape[2] - 1
    sizes = tuple(lax.axis_size(a) for a in AXES)
    vmem = pl.BlockSpec(memory_space=pltpu.VMEM)
    lines = 2 * REACH + 2 * (sizes[0] // 2 // REACH - 1)
    dma = pltpu.SemaphoreType.DMA
    return pl.pallas_call(
        functools.partial(export_kernel, sizes),
        out_shape=(
            jax.ShapeDtypeStruct((ny, nz, 3, slots), jnp.float32),
            jax.ShapeDtypeStruct((8, 128), jnp.float32),
        ),
        in_specs=[vmem, vmem],
        out_specs=(vmem, vmem),
        scratch_shapes=[
            pltpu.VMEM((1 if y else ny, 1 if z else nz, 8, slots), jnp.float32) for _, y, z in CORNERS
        ]
        + [
            pltpu.VMEM((sizes[0], 8, 128), jnp.float32),
            pltpu.VMEM((8, 128), jnp.float32),
            pltpu.VMEM((sizes[1] * sizes[2], 8, 128), jnp.float32),
            dma((len(CORNERS),)),
            dma((len(CORNERS),)),
            dma((lines,)),
            dma((lines,)),
            dma((sizes[1] * sizes[2],)),
            dma((sizes[1] * sizes[2],)),
        ],
        compiler_params=pltpu.CompilerParams(collective_id=1, has_side_effects=True),
    )(forces, energy)


def on_device(coords, charges, atom_types, counts, c6_table, c12_table):
    ny, nz, slots = coords.shape[1], coords.shape[2], coords.shape[4]
    filled = jnp.arange(slots, dtype=jnp.int32) < counts[..., None]
    own = jnp.concatenate(
        [
            coords,
            jnp.where(filled, charges, 0.0)[..., None, :],
            jnp.where(filled, atom_types, 64).astype(jnp.float32)[..., None, :],
            jnp.broadcast_to(counts.astype(jnp.float32)[..., None, None], counts.shape + (1, slots)),
            jnp.zeros(counts.shape + (2, slots), jnp.float32),
        ],
        axis=3,
    )[0]
    raw = import_cells(own)
    types = c6_table.shape[0]
    both = jnp.stack([0.5 * (c6_table + c6_table.T), 0.5 * (c12_table + c12_table.T)], axis=1)
    both = jnp.concatenate([both, both], axis=2)
    both = jnp.pad(both, ((0, 128 - types), (0, 0), (0, 0))).reshape(128, 256)
    high = lax.reduce_precision(both, 8, 7)
    table = jnp.concatenate([high, both - high]).astype(jnp.bfloat16)
    lists = tuple(jnp.asarray(k) for k in neighbour_lists(ny, nz))
    forces, energy = pair_forces(lists, raw, table)
    total, energy_sum = export(forces, energy, slots)
    return (total[None], energy_sum[0, :1])


def solution(mesh):
    return jax.shard_map(
        on_device,
        mesh=mesh,
        in_specs=(
            P(("groups", "gx"), "gy", "gz", None, None),
            P(("groups", "gx"), "gy", "gz", None),
            P(("groups", "gx"), "gy", "gz", None),
            P(("groups", "gx"), "gy", "gz"),
            P(),
            P(),
        ),
        out_specs=(P(("groups", "gx"), "gy", "gz", None, None), P("groups")),
        check_vma=False,
    )
```
